256 devices in a mesh: ep: 64 (over z, y, core), fsdp: 4 (over x).
Axes of the slice: x: 4, y: 4, z: 8, core: 2. Of those that a mesh axis runs over, the one named last changes fastest.
Arguments:
- train_gate: float32 [64, 2048, 1024], P('ep', 'fsdp'), may hold values from -0.1875 to 0.1875
- other_gate: bfloat16 [64, 2048, 1024], P('ep', 'fsdp'), may hold values from -0.0625 to 0.0625
- train_up: float32 [64, 2048, 1024], P('ep', 'fsdp'), may hold values from -0.1875 to 0.1875
- other_up: bfloat16 [64, 2048, 1024], P('ep', 'fsdp'), may hold values from -0.0625 to 0.0625
- router_weight: float32 [2048, 64], P('fsdp', 'ep'), may hold values from -0.125 to 0.125
- router_gain: float32 [2048], P('fsdp'), may hold values from 0.25 to 1.75
Outputs:
- ready_gate: bfloat16 [64, 2048, 1024], P('ep')
- ready_up: bfloat16 [64, 2048, 1024], P('ep')
- scale_gate: float32 [64, 1024], P('ep')
- scale_up: float32 [64, 1024], P('ep')
- serve_router: bfloat16 [2048, 64], replicated
The draws below stay inside these ranges and needn't reach their ends.
All inputs are finite; a program needn't handle non-finite values.
Results may differ from the reference program's by a relative error of at most 0.001.
Values may be sent and summed in bfloat16 or wider, within the bound.
A program may use at most 64 MiB of HBM per device.

```python
import jax
import jax.numpy as jnp
from jax import lax

EXPERTS = 64
D_MODEL = 2048
D_EXPERT = 1024


def strengthened(drawn, key, source, target, shards_of, factor):
    owner, partner = [(jnp.arange(drawn.shape[dim]) // (drawn.shape[dim] // shards_of)).reshape([-1 if axis == dim else 1 for axis in range(drawn.ndim)]) for dim in (source, target)]
    chosen = jax.random.permutation(key, shards_of)[partner]
    strong = (owner == chosen) | (owner == (partner + shards_of // 2) % shards_of)
    return jnp.where(strong, factor * drawn, drawn)


def shard_levels(stream_key, dims, pieces, low, top_value):
    level = 1.0
    for dim, shards_of in pieces:
        steps = jax.random.uniform(jax.random.fold_in(jax.random.fold_in(stream_key, 6), dim), (shards_of,), jnp.float32, low / len(pieces), top_value / len(pieces))
        level = level * jnp.repeat(jnp.exp(steps), dims[dim] // shards_of).reshape((-1,) + (1,) * (len(dims) - 1 - dim))
    return level


def normal_values(own_key, extent, width, most, split=(), dtype=jnp.bfloat16):
    factor_of = shard_levels(own_key, extent, split, -0.22, 0.18) if split else 1.0
    result = jax.random.normal(own_key, extent, jnp.float32) * width * factor_of
    return jnp.minimum(jnp.maximum(result, -most), most).astype(dtype)


def gaussian_with(key, extent, deviation, most, cuts, heavy, held_as=jnp.bfloat16):
    array = deviation * jax.random.normal(key, extent, jnp.float32)
    if cuts:
        array = array * shard_levels(key, extent, cuts, -0.22, 0.18)
    return jnp.clip(strengthened(array, jax.random.fold_in(key, 3), *heavy), -most, most).astype(held_as)


def setup_inputs(seed: int = 0) -> dict:
    streams_of = jax.random.split(jax.random.key(seed), 7)
    return {
        "train_gate": gaussian_with(streams_of[0], (EXPERTS, D_MODEL, D_EXPERT), D_MODEL ** -0.5, 0.1875, ((0, 64), (1, 4)), (1, 2, 4, 2.0), jnp.float32),
        "other_gate": normal_values(streams_of[1], (EXPERTS, D_MODEL, D_EXPERT), (D_MODEL * 4) ** -0.5, 0.0625, ((0, 64), (1, 4))),
        "train_up": gaussian_with(streams_of[2], (EXPERTS, D_MODEL, D_EXPERT), D_MODEL ** -0.5, 0.1875, ((0, 64), (1, 4)), (1, 2, 4, 2.0), jnp.float32),
        "other_up": normal_values(streams_of[3], (EXPERTS, D_MODEL, D_EXPERT), (D_MODEL * 4) ** -0.5, 0.0625, ((0, 64), (1, 4))),
        "router_weight": normal_values(streams_of[4], (D_MODEL, EXPERTS), D_MODEL ** -0.5, 0.125, ((0, 4), (1, 64)), jnp.float32),
        "router_gain": jnp.clip(1.0 + 0.15 * jax.random.normal(streams_of[5], (D_MODEL,), jnp.float32), 0.25, 1.75),
    }


def reference(train_gate, other_gate, train_up, other_up, router_weight, router_gain):
    latest_gate = train_gate + other_gate.astype(jnp.float32)
    latest_up = train_up + other_up.astype(jnp.float32)
    scale_gate = jnp.sqrt(lax.optimization_barrier(jnp.sum(latest_gate * latest_gate, axis=1)))
    ready_gate = (latest_gate / jnp.expand_dims(scale_gate, 1)).astype(jnp.bfloat16)
    scale_up = jnp.sqrt(lax.optimization_barrier(jnp.sum(latest_up * latest_up, axis=1)))
    ready_up = (latest_up / jnp.expand_dims(scale_up, 1)).astype(jnp.bfloat16)
    serve_router = (router_weight * router_gain[:, None]).astype(jnp.bfloat16)
    return (ready_gate, ready_up, scale_gate, scale_up, serve_router)
```

```python
import functools

import jax
import jax.numpy as jnp
from jax import lax
from jax.experimental import pallas as pl
from jax.experimental.pallas import tpu as pltpu
from jax.sharding import PartitionSpec as P

MESH = pl.DeviceIdType.MESH
CHUNKS = 4
STEP = 16


def kernel(
    dims,
    tg_hbm, og_hbm, tu_hbm, ou_hbm, rw_ref, rg_ref,
    out_g, out_u, scale_g, scale_u, router,
    lat, oth, sums, rx, plane, zring,
    in_sem, sum_send, sum_recv, rx_send, rx_recv,
    own_send, own_recv, fwd_send, fwd_recv,
    pl_send, pl_recv, z_send, z_recv,
):
    nx, ny, nz, nc, rows = dims
    x = lax.axis_index("fsdp")
    e = lax.axis_index("ep")
    core = lax.rem(e, nc)
    y = lax.rem(lax.div(e, nc), ny)
    z = lax.div(e, nc * ny)

    def ep_of(zz, yy, cc):
        return (zz * ny + yy) * nc + cc

    def step(v, d, n):
        return lax.rem(v + d + n, n)

    right = (e, step(x, 1, nx))
    left = (e, step(x, -1, nx))
    across = (e, step(x, 2, nx))
    y_up = (ep_of(z, step(y, 1, ny), core), x)
    y_dn = (ep_of(z, step(y, -1, ny), core), x)
    z_up = (ep_of(step(z, 1, nz), y, core), x)
    z_dn = (ep_of(step(z, -1, nz), y, core), x)
    twin = (ep_of(z, y, step(core, 1, nc)), x)
    peers = (right, left, across, y_up, y_dn, z_up, z_dn, twin)

    barrier = pltpu.get_barrier_semaphore()
    for peer in peers:
        pl.semaphore_signal(barrier, inc=1, device_id=peer, device_id_type=MESH)

    size = rows // CHUNKS
    loads = []
    for t, (train, other) in enumerate(((tg_hbm, og_hbm), (tu_hbm, ou_hbm))):
        for c in range(CHUNKS):
            part = pl.ds(c * size, size)
            pair = (
                pltpu.make_async_copy(train.at[0, part], lat.at[t, part], in_sem.at[t, c, 0]),
                pltpu.make_async_copy(other.at[0, part], oth.at[t, part], in_sem.at[t, c, 1]),
            )
            for copy in pair:
                copy.start()
            loads.append(pair)

    def remote(src, dst, send, recv, peer):
        return pltpu.make_async_remote_copy(
            src_ref=src, dst_ref=dst, send_sem=send, recv_sem=recv,
            device_id=peer, device_id_type=MESH,
        )

    def local_sum(t):
        acc = jnp.zeros((8, lat.shape[2]), jnp.float32)
        for c in range(CHUNKS):
            for copy in loads[t * CHUNKS + c]:
                copy.wait()

            def add(i, acc, c=c):
                r = pl.multiple_of(c * size + i * STEP, STEP)
                v = lat[t, pl.ds(r, STEP), :] + oth[t, pl.ds(r, STEP), :].astype(jnp.float32)
                lat[t, pl.ds(r, STEP), :] = v
                v = v * v
                for k in range(STEP // 8):
                    acc = acc + v[8 * k : 8 * k + 8]
                return acc

            acc = lax.fori_loop(0, size // STEP, add, acc)
        return jnp.sum(acc, axis=0, keepdims=True)

    def spread(buf, send, recv):
        copies = []
        for k, peer in enumerate((right, left, across)):
            copy = remote(buf.at[x], buf.at[x], send.at[k], recv.at[k], peer)
            copy.start()
            copies.append(copy)
        return copies

    sums[0, x] = local_sum(0)
    pl.semaphore_wait(barrier, len(peers))
    pending = spread(sums.at[0], sum_send.at[0], sum_recv.at[0])
    rx[x] = rw_ref[...] * rg_ref[...]
    rx_copies = spread(rx, rx_send, rx_recv)
    sums[1, x] = local_sum(1)
    later = spread(sums.at[1], sum_send.at[1], sum_recv.at[1])

    outs, scales = (out_g, out_u), (scale_g, scale_u)
    own = []
    for t in range(2):
        for copy in (pending, later)[t]:
            copy.wait()
        total = sums[t, 0]
        for k in range(1, nx):
            total = total + sums[t, k]
        scale = jnp.sqrt(total)
        scales[t][...] = scale
        inv = jnp.broadcast_to(1.0 / scale, (STEP, lat.shape[2]))
        for c in range(CHUNKS):

            def narrow(i, carry, t=t, c=c, inv=inv):
                r = pl.multiple_of(c * size + i * STEP, STEP)
                w = pl.multiple_of(x * rows + c * size + i * STEP, STEP)
                outs[t][0, pl.ds(w, STEP), :] = (lat[t, pl.ds(r, STEP), :] * inv).astype(jnp.bfloat16)
                return carry

            lax.fori_loop(0, size // STEP, narrow, 0)
            where = pl.ds(pl.multiple_of(x * rows + c * size, size), size)
            piece = outs[t].at[0, where]
            for d, peer in enumerate((right, left)):
                copy = remote(piece, piece, own_send.at[d, t, c], own_recv.at[d, t, c], peer)
                copy.start()
                own.append(copy)

    for copy in rx_copies:
        copy.wait()
    mine = y * nc + core
    plane[mine] = jnp.concatenate([rx[k] for k in range(nx)], axis=1)
    first = remote(plane.at[mine], plane.at[mine], pl_send.at[0], pl_recv.at[0], twin)
    first.start()
    first.wait()
    near = pl.ds(y * nc, nc)
    ups = remote(plane.at[near], plane.at[near], pl_send.at[1], pl_recv.at[1], y_up)
    dns = remote(plane.at[near], plane.at[near], pl_send.at[2], pl_recv.at[2], y_dn)
    ups.start()
    dns.start()
    ups.wait()
    dns.wait()
    from_dn = pl.ds(step(y, -1, ny) * nc, nc)
    far = remote(plane.at[from_dn], plane.at[from_dn], pl_send.at[3], pl_recv.at[3], y_up)
    far.start()
    far.wait()
    zring[z] = jnp.concatenate([plane[k] for k in range(ny * nc)], axis=0)
    hops_up, hops_dn = nz // 2, nz - 1 - nz // 2
    for s in range(hops_up):
        at = step(z, -s, nz)
        moves = [remote(zring.at[at], zring.at[at], z_send.at[0, s], z_recv.at[0, s], z_up)]
        if s < hops_dn:
            at = step(z, s, nz)
            moves.append(remote(zring.at[at], zring.at[at], z_send.at[1, s], z_recv.at[1, s], z_dn))
        for copy in moves:
            copy.start()
        for copy in moves:
            copy.wait()
    for k in range(nz // 2):
        both = jnp.concatenate([zring[2 * k], zring[2 * k + 1]], axis=0)
        router[pl.ds(2 * k * ny * nc, 2 * ny * nc), :] = both.astype(jnp.bfloat16)

    fwd = []
    half = CHUNKS // 2
    for t in range(2):
        for c in range(CHUNKS):
            d = 0 if c < half else 1
            own[(t * CHUNKS + c) * 2 + d].wait_recv()
            source = step(x, -1, nx) if d == 0 else step(x, 1, nx)
            where = pl.ds(pl.multiple_of(source * rows + c * size, size), size)
            piece = outs[t].at[0, where]
            copy = remote(piece, piece, fwd_send.at[t, c], fwd_recv.at[t, c], (right, left)[d])
            copy.start()
            fwd.append(copy)
    for t in range(2):
        for c in range(CHUNKS):
            d = 0 if c < half else 1
            own[(t * CHUNKS + c) * 2 + 1 - d].wait_recv()
    for copy in own:
        copy.wait_send()
    for copy in fwd:
        copy.wait()


def body(dims, train_gate, other_gate, train_up, other_up, router_weight, router_gain):
    nx, ny, nz, nc, rows = dims
    width = train_gate.shape[2]
    whole = nx * rows
    experts = ny * nz * nc
    hbm = pl.BlockSpec(memory_space=pltpu.HBM)
    vmem = pl.BlockSpec(memory_space=pltpu.VMEM)
    dma = pltpu.SemaphoreType.DMA
    out = pl.pallas_call(
        functools.partial(kernel, dims),
        out_shape=(
            pltpu.VMEM((1, whole, width), jnp.bfloat16),
            pltpu.VMEM((1, whole, width), jnp.bfloat16),
            jax.ShapeDtypeStruct((1, width), jnp.float32),
            jax.ShapeDtypeStruct((1, width), jnp.float32),
            jax.ShapeDtypeStruct((experts, whole), jnp.bfloat16),
        ),
        in_specs=[hbm] * 4 + [vmem] * 2,
        out_specs=(vmem,) * 5,
        scratch_shapes=[
            pltpu.VMEM((2, rows, width), jnp.float32),
            pltpu.VMEM((2, rows, width), jnp.bfloat16),
            pltpu.VMEM((2, nx, 1, width), jnp.float32),
            pltpu.VMEM((nx, 1, rows), jnp.float32),
            pltpu.VMEM((ny * nc, 1, whole), jnp.float32),
            pltpu.VMEM((nz, ny * nc, whole), jnp.float32),
            dma((2, CHUNKS, 2)),
            dma((2, 3)), dma((2, 3)), dma((3,)), dma((3,)),
            dma((2, 2, CHUNKS)), dma((2, 2, CHUNKS)), dma((2, CHUNKS)), dma((2, CHUNKS)),
            dma((4,)), dma((4,)), dma((2, 4)), dma((2, 4)),
        ],
        compiler_params=pltpu.CompilerParams(
            collective_id=0, has_side_effects=True, vmem_limit_bytes=48 << 20
        ),
        name="ring",
    )(train_gate, other_gate, train_up, other_up, router_weight.T, router_gain[None, :])
    ready_gate, ready_up, scale_gate, scale_up, router = out
    return ready_gate, ready_up, scale_gate, scale_up, router.T


def solution(mesh):
    placed = (
        P("ep", "fsdp", None),
        P("ep", "fsdp", None),
        P("ep", "fsdp", None),
        P("ep", "fsdp", None),
        P("fsdp", "ep"),
        P("fsdp"),
    )
    nx, ep = mesh.shape["fsdp"], mesh.shape["ep"]
    dims = (nx, 4, ep // 8, 2, 2048 // nx)
    return jax.shard_map(
        functools.partial(body, dims),
        mesh=mesh,
        in_specs=placed,
        out_specs=(P("ep", None, None), P("ep", None, None), P("ep", None), P("ep", None), P()),
        check_vma=False,
    )
```

```python
import functools

import jax
import jax.numpy as jnp
from jax import lax
from jax.experimental import pallas as pl
from jax.experimental.pallas import tpu as pltpu
from jax.sharding import PartitionSpec as P

MESH = pl.DeviceIdType.MESH
CHUNKS = 4
STEP = 16
PARTS = 4


def kernel(
    dims,
    tg_hbm, og_hbm, tu_hbm, ou_hbm, rw_ref, rg_ref,
    out_g, out_u, scale_g, scale_u, router,
    lat, oth, sums, rx, plane, zring,
    in_sem, sum_send, sum_recv, rx_send, rx_recv,
    own_send, own_recv, fwd_send, fwd_recv,
    pl_send, pl_recv, z_send, z_recv,
):
    nx, ny, nz, nc, rows = dims
    x = lax.axis_index("fsdp")
    e = lax.axis_index("ep")
    core = lax.rem(e, nc)
    y = lax.rem(lax.div(e, nc), ny)
    z = lax.div(e, nc * ny)

    def ep_of(zz, yy, cc):
        return (zz * ny + yy) * nc + cc

    def step(v, d, n):
        return lax.rem(v + d + n, n)

    right = (e, step(x, 1, nx))
    left = (e, step(x, -1, nx))
    across = (e, step(x, 2, nx))
    y_up = (ep_of(z, step(y, 1, ny), core), x)
    y_dn = (ep_of(z, step(y, -1, ny), core), x)
    z_up = (ep_of(step(z, 1, nz), y, core), x)
    z_dn = (ep_of(step(z, -1, nz), y, core), x)
    twin = (ep_of(z, y, step(core, 1, nc)), x)
    row = (right, left, across)
    grid = (y_up, y_dn, z_up, z_dn)

    barrier = pltpu.get_barrier_semaphore()
    odd = lax.rem(y + z, 2)

    def greet(them):
        for peer in them:
            pl.semaphore_signal(barrier, inc=1, device_id=peer, device_id_type=MESH)

    greet(row)

    size = rows // CHUNKS
    loads = []
    for t, (train, other) in enumerate(((tg_hbm, og_hbm), (tu_hbm, ou_hbm))):
        for c in range(CHUNKS):
            part = pl.ds(c * size, size)
            pair = (
                pltpu.make_async_copy(train.at[0, part], lat.at[t, part], in_sem.at[t, c, 0]),
                pltpu.make_async_copy(other.at[0, part], oth.at[t, part], in_sem.at[t, c, 1]),
            )
            for copy in pair:
                copy.start()
            loads.append(pair)

    def remote(src, dst, send, recv, peer):
        return pltpu.make_async_remote_copy(
            src_ref=src, dst_ref=dst, send_sem=send, recv_sem=recv,
            device_id=peer, device_id_type=MESH,
        )

    def local_sum(t):
        acc = jnp.zeros((8, lat.shape[2]), jnp.float32)
        for c in range(CHUNKS):
            for copy in loads[t * CHUNKS + c]:
                copy.wait()

            def add(i, acc, c=c):
                r = pl.multiple_of(c * size + i * STEP, STEP)
                v = lat[t, pl.ds(r, STEP), :] + oth[t, pl.ds(r, STEP), :].astype(jnp.float32)
                lat[t, pl.ds(r, STEP), :] = v
                v = v * v
                for k in range(STEP // 8):
                    acc = acc + v[8 * k : 8 * k + 8]
                return acc

            acc = lax.fori_loop(0, size // STEP, add, acc)
        return jnp.sum(acc, axis=0, keepdims=True)

    def spread(buf, send, recv):
        copies = []
        for k, peer in enumerate((right, left, across)):
            copy = remote(buf.at[x], buf.at[x], send.at[k], recv.at[k], peer)
            copy.start()
            copies.append(copy)
        return copies

    sums[0, x] = local_sum(0)
    pl.semaphore_wait(barrier, len(row) + len(grid) * odd + core)
    greet(grid + (twin,))
    pending = spread(sums.at[0], sum_send.at[0], sum_recv.at[0])
    rx[x] = rw_ref[...] * rg_ref[...]
    rx_copies = spread(rx, rx_send, rx_recv)
    sums[1, x] = local_sum(1)
    later = spread(sums.at[1], sum_send.at[1], sum_recv.at[1])

    outs, scales = (out_g, out_u), (scale_g, scale_u)
    own = []
    for t in range(2):
        for copy in (pending, later)[t]:
            copy.wait()
        total = sums[t, 0]
        for k in range(1, nx):
            total = total + sums[t, k]
        scale = jnp.sqrt(total)
        scales[t][...] = scale
        inv = jnp.broadcast_to(1.0 / scale, (STEP, lat.shape[2]))
        for c in range(CHUNKS):

            def narrow(i, carry, t=t, c=c, inv=inv):
                r = pl.multiple_of(c * size + i * STEP, STEP)
                w = pl.multiple_of(x * rows + c * size + i * STEP, STEP)
                outs[t][0, pl.ds(w, STEP), :] = (lat[t, pl.ds(r, STEP), :] * inv).astype(jnp.bfloat16)
                return carry

            lax.fori_loop(0, size // STEP, narrow, 0)
            where = pl.ds(pl.multiple_of(x * rows + c * size, size), size)
            piece = outs[t].at[0, where]
            for d, peer in enumerate((right, left)):
                copy = remote(piece, piece, own_send.at[d, t, c], own_recv.at[d, t, c], peer)
                copy.start()
                own.append(copy)

    answers = len(grid) * (1 - odd) + (1 - core)

    @pl.when(answers > 0)
    def _():
        pl.semaphore_wait(barrier, answers)

    for copy in rx_copies:
        copy.wait()
    mine = y * nc + core
    plane[mine] = jnp.concatenate([rx[k] for k in range(nx)], axis=1)
    first = remote(plane.at[mine], plane.at[mine], pl_send.at[0], pl_recv.at[0], twin)
    first.start()
    first.wait()
    near = pl.ds(y * nc, nc)
    ups = remote(plane.at[near], plane.at[near], pl_send.at[1], pl_recv.at[1], y_up)
    dns = remote(plane.at[near], plane.at[near], pl_send.at[2], pl_recv.at[2], y_dn)
    ups.start()
    dns.start()
    ups.wait()
    dns.wait()
    from_dn = pl.ds(step(y, -1, ny) * nc, nc)
    far = remote(plane.at[from_dn], plane.at[from_dn], pl_send.at[3], pl_recv.at[3], y_up)
    far.start()
    far.wait()
    zring[z] = jnp.concatenate([plane[k] for k in range(ny * nc)], axis=0)
    hops_up, hops_dn = nz // 2, nz - 1 - nz // 2
    for s in range(hops_up):
        at = step(z, -s, nz)
        moves = [remote(zring.at[at], zring.at[at], z_send.at[0, s], z_recv.at[0, s], z_up)]
        if s < hops_dn:
            at = step(z, s, nz)
            moves.append(remote(zring.at[at], zring.at[at], z_send.at[1, s], z_recv.at[1, s], z_dn))
        for copy in moves:
            copy.start()
        for copy in moves:
            copy.wait()
    for k in range(nz // 2):
        both = jnp.concatenate([zring[2 * k], zring[2 * k + 1]], axis=0)
        router[pl.ds(2 * k * ny * nc, 2 * ny * nc), :] = both.astype(jnp.bfloat16)

    fwd = []
    half = CHUNKS // 2
    for t in range(2):
        for c in range(CHUNKS):
            d = 0 if c < half else 1
            own[(t * CHUNKS + c) * 2 + d].wait_recv()
            source = step(x, -1, nx) if d == 0 else step(x, 1, nx)
            where = pl.ds(pl.multiple_of(source * rows + c * size, size), size)
            piece = outs[t].at[0, where]
            copy = remote(piece, piece, fwd_send.at[t, c], fwd_recv.at[t, c], (right, left)[d])
            copy.start()
            fwd.append(copy)
    for t in range(2):
        for c in range(CHUNKS):
            d = 0 if c < half else 1
            own[(t * CHUNKS + c) * 2 + 1 - d].wait_recv()
    for copy in own:
        copy.wait_send()
    for copy in fwd:
        copy.wait()


def write_out(*refs):
    held, outs, sem = refs[:5], refs[5:10], refs[10]
    copies = []
    for k in range(2):
        size = held[k].shape[1] // PARTS
        for p in range(PARTS):
            part = (0, pl.ds(p * size, size))
            copies.append(pltpu.make_async_copy(held[k].at[part], outs[k].at[part], sem.at[k, p]))
    for k in range(2, 5):
        copies.append(pltpu.make_async_copy(held[k], outs[k], sem.at[k, 0]))
    for copy in copies:
        copy.start()
    for copy in copies:
        copy.wait()


def body(dims, train_gate, other_gate, train_up, other_up, router_weight, router_gain):
    nx, ny, nz, nc, rows = dims
    width = train_gate.shape[2]
    whole = nx * rows
    experts = ny * nz * nc
    hbm = pl.BlockSpec(memory_space=pltpu.HBM)
    vmem = pl.BlockSpec(memory_space=pltpu.VMEM)
    dma = pltpu.SemaphoreType.DMA
    out = pl.pallas_call(
        functools.partial(kernel, dims),
        out_shape=(
            pltpu.VMEM((1, whole, width), jnp.bfloat16),
            pltpu.VMEM((1, whole, width), jnp.bfloat16),
            pltpu.VMEM((1, width), jnp.float32),
            pltpu.VMEM((1, width), jnp.float32),
            pltpu.VMEM((experts, whole), jnp.bfloat16),
        ),
        in_specs=[hbm] * 4 + [vmem] * 2,
        out_specs=(vmem,) * 5,
        scratch_shapes=[
            pltpu.VMEM((2, rows, width), jnp.float32),
            pltpu.VMEM((2, rows, width), jnp.bfloat16),
            pltpu.VMEM((2, nx, 1, width), jnp.float32),
            pltpu.VMEM((nx, 1, rows), jnp.float32),
            pltpu.VMEM((ny * nc, 1, whole), jnp.float32),
            pltpu.VMEM((nz, ny * nc, whole), jnp.float32),
            dma((2, CHUNKS, 2)),
            dma((2, 3)), dma((2, 3)), dma((3,)), dma((3,)),
            dma((2, 2, CHUNKS)), dma((2, 2, CHUNKS)), dma((2, CHUNKS)), dma((2, CHUNKS)),
            dma((4,)), dma((4,)), dma((2, 4)), dma((2, 4)),
        ],
        compiler_params=pltpu.CompilerParams(
            collective_id=0, has_side_effects=True, vmem_limit_bytes=48 << 20
        ),
        name="ring",
    )(train_gate, other_gate, train_up, other_up, router_weight.T, router_gain[None, :])
    ready_gate, ready_up, scale_gate, scale_up, router = pl.pallas_call(
        write_out,
        out_shape=tuple(jax.ShapeDtypeStruct(o.shape, o.dtype) for o in out),
        in_specs=[vmem] * 5,
        out_specs=(hbm,) * 5,
        scratch_shapes=[dma((5, PARTS))],
        compiler_params=pltpu.CompilerParams(vmem_limit_bytes=4 << 20),
        name="write_out",
    )(*out)
    return ready_gate, ready_up, scale_gate, scale_up, router.T


def solution(mesh):
    placed = (
        P("ep", "fsdp", None),
        P("ep", "fsdp", None),
        P("ep", "fsdp", None),
        P("ep", "fsdp", None),
        P("fsdp", "ep"),
        P("fsdp"),
    )
    nx, ep = mesh.shape["fsdp"], mesh.shape["ep"]
    dims = (nx, 4, ep // 8, 2, 2048 // nx)
    return jax.shard_map(
        functools.partial(body, dims),
        mesh=mesh,
        in_specs=placed,
        out_specs=(P("ep", None, None), P("ep", None, None), P("ep", None), P("ep", None), P()),
        check_vma=False,
    )
```

```python
import functools

import jax
import jax.numpy as jnp
from jax import lax
from jax.experimental import pallas as pl
from jax.experimental.pallas import tpu as pltpu
from jax.sharding import PartitionSpec as P

MESH = pl.DeviceIdType.MESH
CHUNKS = 4
STEP = 16
PARTS = 4
RAW = 64
SPLIT = 2


def kernel(
    dims,
    tg_hbm, og_hbm, tu_hbm, ou_hbm, rw_ref, rg_ref,
    out_g, out_u, scale_g, scale_u, router,
    lat, oth, sums, raw, rx, plane, zring,
    in_sem, sum_send, sum_recv, raw_send, raw_recv, rx_send, rx_recv,
    own_send, own_recv, fwd_send, fwd_recv,
    pl_send, pl_recv, z_send, z_recv, answer_sem,
):
    nx, ny, nz, nc, rows = dims
    width = lat.shape[2]
    x = lax.axis_index("fsdp")
    e = lax.axis_index("ep")
    core = lax.rem(e, nc)
    y = lax.rem(lax.div(e, nc), ny)
    z = lax.div(e, nc * ny)
    y_odd, z_odd = lax.rem(y, 2), lax.rem(z, 2)

    def ep_of(zz, yy, cc):
        return (zz * ny + yy) * nc + cc

    def step(v, d, n):
        return lax.rem(v + d + n, n)

    def remote(src, dst, send, recv, peer):
        return pltpu.make_async_remote_copy(
            src_ref=src, dst_ref=dst, send_sem=send, recv_sem=recv,
            device_id=peer, device_id_type=MESH,
        )

    right = (e, step(x, 1, nx))
    left = (e, step(x, -1, nx))
    across = (e, step(x, 2, nx))
    y_up = (ep_of(z, step(y, 1, ny), core), x)
    y_dn = (ep_of(z, step(y, -1, ny), core), x)
    z_up = (ep_of(step(z, 1, nz), y, core), x)
    z_dn = (ep_of(step(z, -1, nz), y, core), x)
    twin = (ep_of(z, y, step(core, 1, nc)), x)

    barrier = pltpu.get_barrier_semaphore()
    for peer in (right, left, across):
        pl.semaphore_signal(barrier, inc=1, device_id=peer, device_id_type=MESH)
    pairs = ((z_odd, (z_up, z_dn)), (y_odd, (y_up, y_dn)), (core, (twin,)))
    for side, them in pairs:

        @pl.when(side == 0)
        def _(them=them):
            for peer in them:
                pl.semaphore_signal(barrier, inc=1, device_id=peer, device_id_type=MESH)

    part = width // SPLIT
    items = [(0, k * part, part) for k in range(SPLIT)] + [(1, 0, width)]
    size = rows // CHUNKS
    loads = []
    for i, (t, col, wide) in enumerate(items):
        train, other = ((tg_hbm, og_hbm), (tu_hbm, ou_hbm))[t]
        for c in range(CHUNKS):
            at = (pl.ds(c * size, size), pl.ds(col, wide))
            pair = (
                pltpu.make_async_copy(train.at[0, *at], lat.at[t, *at], in_sem.at[i, c, 0]),
                pltpu.make_async_copy(other.at[0, *at], oth.at[t, *at], in_sem.at[i, c, 1]),
            )
            for copy in pair:
                copy.start()
            loads.append(pair)

    def local_sum(i):
        t, col, wide = items[i]
        cols = pl.ds(col, wide)
        acc = jnp.zeros((8, wide), jnp.float32)
        for c in range(CHUNKS):
            for copy in loads[i * CHUNKS + c]:
                copy.wait()

            def add(j, acc, c=c):
                r = pl.ds(pl.multiple_of(c * size + j * STEP, STEP), STEP)
                v = lat[t, r, cols] + oth[t, r, cols].astype(jnp.float32)
                lat[t, r, cols] = v
                v = v * v
                for k in range(STEP // 8):
                    acc = acc + v[8 * k : 8 * k + 8]
                return acc

            acc = lax.fori_loop(0, size // STEP, add, acc)
        sums[t, x, :, cols] = jnp.sum(acc, axis=0, keepdims=True)

    def spread(piece, send, recv):
        copies = []
        for k, peer in enumerate((across, right, left)):
            copy = remote(piece, piece, send.at[k], recv.at[k], peer)
            copy.start()
            copies.append(copy)
        return copies

    sum_copies = []

    def send_sum(i):
        t, col, wide = items[i]
        sum_copies.append(spread(sums.at[t, x, :, pl.ds(col, wide)], sum_send.at[i], sum_recv.at[i]))

    local_sum(0)
    pl.semaphore_wait(barrier, 3 + 2 * z_odd + 2 * y_odd + core)
    send_sum(0)
    raw_at = (pl.ds(0, RAW), pl.ds(items[0][1], items[0][2]))
    raw_copies = []
    for d, peer in enumerate((right, left)):
        copy = remote(lat.at[0, *raw_at], raw.at[d], raw_send.at[d], raw_recv.at[d], peer)
        copy.start()
        raw_copies.append(copy)
    for side, them in pairs:

        @pl.when(side == 1)
        def _(them=them):
            for peer in them:
                pl.semaphore_signal(answer_sem, inc=1, device_id=peer, device_id_type=MESH)

    rx[x] = rw_ref[...] * rg_ref[...]
    rx_copies = spread(rx.at[x], rx_send, rx_recv)
    for i in range(1, len(items)):
        local_sum(i)
        send_sum(i)

    outs, scales = (out_g, out_u), (scale_g, scale_u)
    own = {}
    inverse = []
    for i, (t, col, wide) in enumerate(items):
        cols = pl.ds(col, wide)
        for copy in sum_copies[i]:
            copy.wait()
        total = sums[t, 0, :, cols]
        for k in range(1, nx):
            total = total + sums[t, k, :, cols]
        scale = jnp.sqrt(total)
        scales[t][:, cols] = scale
        inv = jnp.broadcast_to(1.0 / scale, (STEP, wide))
        inverse.append(inv)
        for c in range(CHUNKS):
            skip = RAW if i == 0 and c == 0 else 0
            for lo, hi in ((skip, size), (0, skip)):
                if lo == hi:
                    continue

                def narrow(j, carry, t=t, c=c, inv=inv, cols=cols):
                    r = pl.multiple_of(c * size + j * STEP, STEP)
                    w = pl.multiple_of(x * rows + c * size + j * STEP, STEP)
                    outs[t][0, pl.ds(w, STEP), cols] = (lat[t, pl.ds(r, STEP), cols] * inv).astype(jnp.bfloat16)
                    return carry

                lax.fori_loop(lo // STEP, hi // STEP, narrow, 0)
                if lo == skip:
                    where = pl.ds(pl.multiple_of(x * rows + c * size + skip, STEP), size - skip)
                    piece = outs[t].at[0, where, cols]
                    for d, peer in enumerate((right, left)):
                        copy = remote(piece, piece, own_send.at[d, i, c], own_recv.at[d, i, c], peer)
                        copy.start()
                        own[d, i, c] = copy

    cols = pl.ds(items[0][1], items[0][2])
    for d, source in enumerate((step(x, -1, nx), step(x, 1, nx))):
        raw_copies[d].wait_recv()

        def narrow_raw(j, carry, d=d, source=source):
            r = pl.multiple_of(j * STEP, STEP)
            w = pl.multiple_of(source * rows + j * STEP, STEP)
            outs[0][0, pl.ds(w, STEP), cols] = (raw[d, pl.ds(r, STEP), :] * inverse[0]).astype(jnp.bfloat16)
            return carry

        lax.fori_loop(0, RAW // STEP, narrow_raw, 0)

    answers = 2 * (1 - z_odd) + 2 * (1 - y_odd) + (1 - core)

    @pl.when(answers > 0)
    def _():
        pl.semaphore_wait(answer_sem, answers)

    for copy in rx_copies:
        copy.wait()
    mine = y * nc + core
    plane[mine] = jnp.concatenate([rx[k] for k in range(nx)], axis=1)
    first = remote(plane.at[mine], plane.at[mine], pl_send.at[0], pl_recv.at[0], twin)
    first.start()
    first.wait()
    near = pl.ds(y * nc, nc)
    ups = remote(plane.at[near], plane.at[near], pl_send.at[1], pl_recv.at[1], y_up)
    dns = remote(plane.at[near], plane.at[near], pl_send.at[2], pl_recv.at[2], y_dn)
    ups.start()
    dns.start()
    ups.wait()
    dns.wait()
    from_dn = pl.ds(step(y, -1, ny) * nc, nc)
    far = remote(plane.at[from_dn], plane.at[from_dn], pl_send.at[3], pl_recv.at[3], y_up)
    far.start()
    far.wait()
    zring[z] = jnp.concatenate([plane[k] for k in range(ny * nc)], axis=0)
    hops_up, hops_dn = nz // 2, nz - 1 - nz // 2
    for s in range(hops_up):
        at = step(z, -s, nz)
        moves = [remote(zring.at[at], zring.at[at], z_send.at[0, s], z_recv.at[0, s], z_up)]
        if s < hops_dn:
            at = step(z, s, nz)
            moves.append(remote(zring.at[at], zring.at[at], z_send.at[1, s], z_recv.at[1, s], z_dn))
        for copy in moves:
            copy.start()
        for copy in moves:
            copy.wait()
    for k in range(nz // 2):
        both = jnp.concatenate([zring[2 * k], zring[2 * k + 1]], axis=0)
        router[pl.ds(2 * k * ny * nc, 2 * ny * nc), :] = both.astype(jnp.bfloat16)

    fwd = []
    half = CHUNKS // 2
    by_tensor = [[i for i, item in enumerate(items) if item[0] == t] for t in range(2)]
    for t in range(2):
        for c in range(CHUNKS):
            d = 0 if c < half else 1
            for i in by_tensor[t]:
                own[d, i, c].wait_recv()
            source = step(x, -1, nx) if d == 0 else step(x, 1, nx)
            where = pl.ds(pl.multiple_of(source * rows + c * size, size), size)
            piece = outs[t].at[0, where]
            copy = remote(piece, piece, fwd_send.at[t, c], fwd_recv.at[t, c], (right, left)[d])
            copy.start()
            fwd.append(copy)
    for t in range(2):
        for c in range(CHUNKS):
            d = 0 if c < half else 1
            for i in by_tensor[t]:
                own[1 - d, i, c].wait_recv()
    for copy in raw_copies + list(own.values()):
        copy.wait_send()
    for copy in fwd:
        copy.wait()


def write_out(*refs):
    held, outs, sem = refs[:5], refs[5:10], refs[10]
    copies = []
    for k in range(2):
        size = held[k].shape[1] // PARTS
        for p in range(PARTS):
            part = (0, pl.ds(p * size, size))
            copies.append(pltpu.make_async_copy(held[k].at[part], outs[k].at[part], sem.at[k, p]))
    for k in range(2, 5):
        copies.append(pltpu.make_async_copy(held[k], outs[k], sem.at[k, 0]))
    for copy in copies:
        copy.start()
    for copy in copies:
        copy.wait()


def body(dims, train_gate, other_gate, train_up, other_up, router_weight, router_gain):
    nx, ny, nz, nc, rows = dims
    width = train_gate.shape[2]
    whole = nx * rows
    experts = ny * nz * nc
    hbm = pl.BlockSpec(memory_space=pltpu.HBM)
    vmem = pl.BlockSpec(memory_space=pltpu.VMEM)
    dma = pltpu.SemaphoreType.DMA
    count = SPLIT + 1
    out = pl.pallas_call(
        functools.partial(kernel, dims),
        out_shape=(
            pltpu.VMEM((1, whole, width), jnp.bfloat16),
            pltpu.VMEM((1, whole, width), jnp.bfloat16),
            pltpu.VMEM((1, width), jnp.float32),
            pltpu.VMEM((1, width), jnp.float32),
            pltpu.VMEM((experts, whole), jnp.bfloat16),
        ),
        in_specs=[hbm] * 4 + [vmem] * 2,
        out_specs=(vmem,) * 5,
        scratch_shapes=[
            pltpu.VMEM((2, rows, width), jnp.float32),
            pltpu.VMEM((2, rows, width), jnp.bfloat16),
            pltpu.VMEM((2, nx, 1, width), jnp.float32),
            pltpu.VMEM((2, RAW, width // SPLIT), jnp.float32),
            pltpu.VMEM((nx, 1, rows), jnp.float32),
            pltpu.VMEM((ny * nc, 1, whole), jnp.float32),
            pltpu.VMEM((nz, ny * nc, whole), jnp.float32),
            dma((count, CHUNKS, 2)),
            dma((count, 3)), dma((count, 3)), dma((2,)), dma((2,)), dma((3,)), dma((3,)),
            dma((2, count, CHUNKS)), dma((2, count, CHUNKS)), dma((2, CHUNKS)), dma((2, CHUNKS)),
            dma((4,)), dma((4,)), dma((2, 4)), dma((2, 4)),
            pltpu.SemaphoreType.REGULAR,
        ],
        compiler_params=pltpu.CompilerParams(
            collective_id=0, has_side_effects=True, vmem_limit_bytes=48 << 20
        ),
        name="ring",
    )(train_gate, other_gate, train_up, other_up, router_weight.T, router_gain[None, :])
    ready_gate, ready_up, scale_gate, scale_up, router = pl.pallas_call(
        write_out,
        out_shape=tuple(jax.ShapeDtypeStruct(o.shape, o.dtype) for o in out),
        in_specs=[vmem] * 5,
        out_specs=(hbm,) * 5,
        scratch_shapes=[dma((5, PARTS))],
        compiler_params=pltpu.CompilerParams(vmem_limit_bytes=4 << 20),
        name="write_out",
    )(*out)
    return ready_gate, ready_up, scale_gate, scale_up, router.T


def solution(mesh):
    placed = (
        P("ep", "fsdp", None),
        P("ep", "fsdp", None),
        P("ep", "fsdp", None),
        P("ep", "fsdp", None),
        P("fsdp", "ep"),
        P("fsdp"),
    )
    nx, ep = mesh.shape["fsdp"], mesh.shape["ep"]
    dims = (nx, 4, ep // 8, 2, 2048 // nx)
    return jax.shard_map(
        functools.partial(body, dims),
        mesh=mesh,
        in_specs=placed,
        out_specs=(P("ep", None, None), P("ep", None, None), P("ep", None), P("ep", None), P()),
        check_vma=False,
    )
```

```python
import functools

import jax
import jax.numpy as jnp
from jax import lax
from jax.experimental import pallas as pl
from jax.experimental.pallas import tpu as pltpu
from jax.sharding import PartitionSpec as P

MESH = pl.DeviceIdType.MESH
STEP = 16
PARTS = 2
RAW = 64
FIRST = 256
PIECES = 2


def kernel(
    dims,
    tg_hbm, og_hbm, tu_hbm, ou_hbm, rw_hbm, rg_hbm,
    out_g, out_u, scale_g, scale_u, router,
    lat, oth, sums, raw, rin, rx, plane, zring,
    in_sem, rin_sem, sum_send, sum_recv, raw_send, raw_recv, rx_send, rx_recv,
    own_send, near_recv, rest_recv, fwd_send, fwd_recv,
    pl_send, pl_recv, z_send, z_recv, answer_sem,
):
    nx, ny, nz, nc, rows = dims
    width = lat.shape[2]
    half = rows // 2
    x = lax.axis_index("fsdp")
    e = lax.axis_index("ep")
    core = lax.rem(e, nc)
    y = lax.rem(lax.div(e, nc), ny)
    z = lax.div(e, nc * ny)
    y_odd, z_odd = lax.rem(y, 2), lax.rem(z, 2)

    def ep_of(zz, yy, cc):
        return (zz * ny + yy) * nc + cc

    def step(v, d, n):
        return lax.rem(v + d + n, n)

    def remote(src, dst, send, recv, peer):
        return pltpu.make_async_remote_copy(
            src_ref=src, dst_ref=dst, send_sem=send, recv_sem=recv,
            device_id=peer, device_id_type=MESH,
        )

    def wait_bytes(ref, sem):
        pltpu.make_async_copy(ref, ref, sem).wait()

    right = (e, step(x, 1, nx))
    left = (e, step(x, -1, nx))
    across = (e, step(x, 2, nx))
    y_up = (ep_of(z, step(y, 1, ny), core), x)
    y_dn = (ep_of(z, step(y, -1, ny), core), x)
    z_up = (ep_of(step(z, 1, nz), y, core), x)
    z_dn = (ep_of(step(z, -1, nz), y, core), x)
    twin = (ep_of(z, y, step(core, 1, nc)), x)

    barrier = pltpu.get_barrier_semaphore()
    for peer in (across, right, left):
        pl.semaphore_signal(barrier, inc=1, device_id=peer, device_id_type=MESH)
    pairs = ((z_odd, (z_up, z_dn)), (y_odd, (y_up, y_dn)), (core, (twin,)))

    items = ((0, 0, FIRST), (0, FIRST, width - FIRST), (1, 0, width))
    loads = []
    for i, (t, col, wide) in enumerate(items):
        train, other = ((tg_hbm, og_hbm), (tu_hbm, ou_hbm))[t]
        for h in range(2):
            at = (pl.ds(h * half, half), pl.ds(col, wide))
            pair = (
                pltpu.make_async_copy(train.at[0, *at], lat.at[t, *at], in_sem.at[i, h, 0]),
                pltpu.make_async_copy(other.at[0, *at], oth.at[t, *at], in_sem.at[i, h, 1]),
            )
            for copy in pair:
                copy.start(priority=min(i, 1))
            loads.append(pair)
        if i == 0:
            pltpu.make_async_copy(rw_hbm, rin.at[0], rin_sem).start()
            pltpu.make_async_copy(rg_hbm, rin.at[1], rin_sem).start()

    for side, them in pairs:

        @pl.when(side == 0)
        def _(them=them):
            for peer in them:
                pl.semaphore_signal(barrier, inc=1, device_id=peer, device_id_type=MESH)

    def local_sum(i):
        t, col, wide = items[i]
        cols = pl.ds(col, wide)
        acc = jnp.zeros((8, wide), jnp.float32)
        for h in range(2):
            for copy in loads[2 * i + h]:
                copy.wait()

            def add(j, acc, h=h):
                r = pl.ds(pl.multiple_of(h * half + j * STEP, STEP), STEP)
                v = lat[t, r, cols] + oth[t, r, cols].astype(jnp.float32)
                lat[t, r, cols] = v
                v = v * v
                for k in range(STEP // 8):
                    acc = acc + v[8 * k : 8 * k + 8]
                return acc

            acc = lax.fori_loop(0, half // STEP, add, acc)
        sums[t, x, :, cols] = jnp.sum(acc, axis=0, keepdims=True)

    def spread(piece, send, recv):
        for peer in (across, right, left):
            remote(piece, piece, send, recv, peer).start()

    def send_sum(i):
        t, col, wide = items[i]
        spread(sums.at[t, x, :, pl.ds(col, wide)], sum_send, sum_recv.at[i])

    local_sum(0)
    pl.semaphore_wait(barrier, 3 + 2 * z_odd + 2 * y_odd + core)
    send_sum(0)
    for d, peer in enumerate((right, left)):
        remote(lat.at[0, pl.ds(0, RAW), pl.ds(0, FIRST)], raw.at[d], raw_send, raw_recv, peer).start()
    for side, them in pairs:

        @pl.when(side == 1)
        def _(them=them):
            for peer in them:
                pl.semaphore_signal(answer_sem, inc=1, device_id=peer, device_id_type=MESH)

    for i in range(1, len(items)):
        local_sum(i)
        send_sum(i)
    wait_bytes(rin, rin_sem)
    rx[x] = rin[0] * rin[1]
    spread(rx.at[x], rx_send, rx_recv)

    outs, scales = (out_g, out_u), (scale_g, scale_u)
    inverse = []
    size = half // PIECES
    for i, (t, col, wide) in enumerate(items):
        cols = pl.ds(col, wide)
        wait_bytes(sums.at[t, pl.ds(0, nx - 1), :, cols], sum_recv.at[i])
        total = sums[t, 0, :, cols]
        for k in range(1, nx):
            total = total + sums[t, k, :, cols]
        scale = jnp.sqrt(total)
        scales[t][:, cols] = scale
        inv = jnp.broadcast_to(1.0 / scale, (STEP, wide))
        inverse.append(inv)
        for c in range(2 * PIECES):
            h = c // PIECES
            skip = RAW if i == 0 and c == 0 else 0
            for lo, hi in ((skip, size), (0, skip)):
                if lo == hi:
                    continue

                def narrow(j, carry, t=t, c=c, inv=inv, cols=cols):
                    r = pl.multiple_of(c * size + j * STEP, STEP)
                    w = pl.multiple_of(x * rows + c * size + j * STEP, STEP)
                    outs[t][0, pl.ds(w, STEP), cols] = (lat[t, pl.ds(r, STEP), cols] * inv).astype(jnp.bfloat16)
                    return carry

                lax.fori_loop(lo // STEP, hi // STEP, narrow, 0)
                if lo == skip:
                    where = pl.ds(pl.multiple_of(x * rows + c * size + skip, STEP), size - skip)
                    piece = outs[t].at[0, where, cols]
                    for d, peer in enumerate((right, left)):
                        recv = near_recv.at[d, t] if h == d else rest_recv.at[d]
                        remote(piece, piece, own_send, recv, peer).start()

    wait_bytes(raw, raw_recv)
    sides = (step(x, -1, nx), step(x, 1, nx))
    for d, source in enumerate(sides):

        def narrow_raw(j, carry, d=d, source=source):
            r = pl.multiple_of(j * STEP, STEP)
            w = pl.multiple_of(source * rows + j * STEP, STEP)
            outs[0][0, pl.ds(w, STEP), pl.ds(0, FIRST)] = (raw[d, pl.ds(r, STEP), :] * inverse[0]).astype(jnp.bfloat16)
            return carry

        lax.fori_loop(0, RAW // STEP, narrow_raw, 0)

    answers = 2 * (1 - z_odd) + 2 * (1 - y_odd) + (1 - core)

    @pl.when(answers > 0)
    def _():
        pl.semaphore_wait(answer_sem, answers)

    wait_bytes(rx.at[pl.ds(0, nx - 1)], rx_recv)
    mine = y * nc + core
    plane[mine] = jnp.concatenate([rx[k] for k in range(nx)], axis=1)
    first = remote(plane.at[mine], plane.at[mine], pl_send, pl_recv.at[0], twin)
    first.start()
    first.wait_recv()
    near = pl.ds(y * nc, nc)
    ups = remote(plane.at[near], plane.at[near], pl_send, pl_recv.at[1], y_up)
    dns = remote(plane.at[near], plane.at[near], pl_send, pl_recv.at[2], y_dn)
    ups.start()
    dns.start()
    ups.wait_recv()
    dns.wait_recv()
    from_dn = pl.ds(step(y, -1, ny) * nc, nc)
    far = remote(plane.at[from_dn], plane.at[from_dn], pl_send, pl_recv.at[3], y_up)
    far.start()
    far.wait_recv()
    zring[z] = jnp.concatenate([plane[k] for k in range(ny * nc)], axis=0)
    hops_up, hops_dn = nz // 2, nz - 1 - nz // 2
    for s in range(hops_up):
        at = step(z, -s, nz)
        moves = [remote(zring.at[at], zring.at[at], z_send, z_recv.at[s], z_up)]
        if s < hops_dn:
            at = step(z, s, nz)
            moves.append(remote(zring.at[at], zring.at[at], z_send, z_recv.at[hops_up + s], z_dn))
        for copy in moves:
            copy.start()
        for copy in moves:
            copy.wait_recv()
    for k in range(nz // 2):
        both = jnp.concatenate([zring[2 * k], zring[2 * k + 1]], axis=0)
        router[pl.ds(2 * k * ny * nc, 2 * ny * nc), :] = both.astype(jnp.bfloat16)

    sent_raw = RAW * FIRST // width
    for t in range(2):
        for d, source in enumerate(sides):
            count = half - (sent_raw if t == 0 and d == 0 else 0)
            wait_bytes(outs[t].at[0, pl.ds(0, count)], near_recv.at[d, t])
            where = pl.ds(pl.multiple_of(source * rows + d * half, half), half)
            piece = outs[t].at[0, where]
            remote(piece, piece, fwd_send, fwd_recv, (right, left)[d]).start()
    for d in range(2):
        count = 2 * half - (sent_raw if d == 1 else 0)
        wait_bytes(out_g.at[0, pl.ds(0, count)], rest_recv.at[d])
    wait_bytes(sums.at[:, pl.ds(0, nx - 1)], sum_send)
    wait_bytes(rx.at[pl.ds(0, nx - 1)], rx_send)
    wait_bytes(raw, raw_send)
    wait_bytes(plane.at[pl.ds(0, 1 + 3 * nc)], pl_send)
    wait_bytes(zring.at[pl.ds(0, nz - 1)], z_send)
    wait_bytes(out_g.at[0, pl.ds(0, 2 * (2 * rows - sent_raw))], own_send)
    wait_bytes(out_g.at[0, pl.ds(0, 4 * half)], fwd_send)
    wait_bytes(out_g.at[0, pl.ds(0, 4 * half)], fwd_recv)


def write_out(*refs):
    held, outs, sem = refs[:5], refs[5:10], refs[10]
    copies = []
    for k in range(2):
        size = held[k].shape[1] // PARTS
        for p in range(PARTS):
            part = (0, pl.ds(p * size, size))
            copies.append(pltpu.make_async_copy(held[k].at[part], outs[k].at[part], sem.at[k * PARTS + p]))
    for k in range(2, 5):
        copies.append(pltpu.make_async_copy(held[k], outs[k], sem.at[2 * PARTS + k - 2]))
    for copy in copies:
        copy.start()
    for copy in copies:
        copy.wait()


def body(dims, train_gate, other_gate, train_up, other_up, router_weight, router_gain):
    nx, ny, nz, nc, rows = dims
    width = train_gate.shape[2]
    whole = nx * rows
    experts = ny * nz * nc
    hbm = pl.BlockSpec(memory_space=pltpu.HBM)
    vmem = pl.BlockSpec(memory_space=pltpu.VMEM)
    dma = pltpu.SemaphoreType.DMA
    out = pl.pallas_call(
        functools.partial(kernel, dims),
        out_shape=(
            pltpu.VMEM((1, whole, width), jnp.bfloat16),
            pltpu.VMEM((1, whole, width), jnp.bfloat16),
            pltpu.VMEM((1, width), jnp.float32),
            pltpu.VMEM((1, width), jnp.float32),
            pltpu.VMEM((experts, whole), jnp.bfloat16),
        ),
        in_specs=[hbm] * 6,
        out_specs=(vmem,) * 5,
        scratch_shapes=[
            pltpu.VMEM((2, rows, width), jnp.float32),
            pltpu.VMEM((2, rows, width), jnp.bfloat16),
            pltpu.VMEM((2, nx, 1, width), jnp.float32),
            pltpu.VMEM((2, RAW, FIRST), jnp.float32),
            pltpu.VMEM((2, 1, rows), jnp.float32),
            pltpu.VMEM((nx, 1, rows), jnp.float32),
            pltpu.VMEM((ny * nc, 1, whole), jnp.float32),
            pltpu.VMEM((nz, ny * nc, whole), jnp.float32),
            dma((3, 2, 2)), dma(()), dma(()), dma((3,)), dma(()), dma(()), dma(()), dma(()),
            dma(()), dma((2, 2)), dma((2,)), dma(()), dma(()),
            dma(()), dma((4,)), dma(()), dma((nz - 1,)),
            pltpu.SemaphoreType.REGULAR,
        ],
        compiler_params=pltpu.CompilerParams(
            collective_id=0, has_side_effects=True, vmem_limit_bytes=48 << 20
        ),
        name="ring",
    )(train_gate, other_gate, train_up, other_up, router_weight.T, router_gain[None, :])
    ready_gate, ready_up, scale_gate, scale_up, router = pl.pallas_call(
        write_out,
        out_shape=tuple(pltpu.HBM(o.shape, o.dtype) for o in out),
        in_specs=[vmem] * 5,
        out_specs=(hbm,) * 5,
        scratch_shapes=[dma((2 * PARTS + 3,))],
        compiler_params=pltpu.CompilerParams(vmem_limit_bytes=4 << 20),
        name="write_out",
    )(*out)
    return ready_gate, ready_up, scale_gate, scale_up, router.T


def solution(mesh):
    placed = (
        P("ep", "fsdp", None),
        P("ep", "fsdp", None),
        P("ep", "fsdp", None),
        P("ep", "fsdp", None),
        P("fsdp", "ep"),
        P("fsdp"),
    )
    nx, ep = mesh.shape["fsdp"], mesh.shape["ep"]
    dims = (nx, 4, ep // 8, 2, 2048 // nx)
    return jax.shard_map(
        functools.partial(body, dims),
        mesh=mesh,
        in_specs=placed,
        out_specs=(P("ep", None, None), P("ep", None, None), P("ep", None), P("ep", None), P()),
        check_vma=False,
    )
```

```python
import functools

import jax
import jax.numpy as jnp
from jax import lax
from jax.experimental import pallas as pl
from jax.experimental.pallas import tpu as pltpu
from jax.sharding import PartitionSpec as P

MESH = pl.DeviceIdType.MESH
STEP = 16
PARTS = 2
RAW = 64
FIRST = 256
PIECES = 2


def kernel(
    dims,
    tg_hbm, og_hbm, tu_hbm, ou_hbm, rw_hbm, rg_hbm,
    out_g, out_u, scale_g, scale_u, router,
    lat, oth, sums, raw, rin, rx, plane, zring,
    in_sem, rin_sem, sum_send, sum_recv, raw_send, raw_recv, rx_send, rx_recv,
    own_send, near_recv, rest_recv, fwd_send, fwd_recv,
    pl_send, pl_recv, z_send, z_recv, answer_sem,
):
    nx, ny, nz, nc, rows = dims
    width = lat.shape[2]
    half = rows // 2
    x = lax.axis_index("fsdp")
    e = lax.axis_index("ep")
    core = lax.rem(e, nc)
    y = lax.rem(lax.div(e, nc), ny)
    z = lax.div(e, nc * ny)

    def ep_of(zz, yy, cc):
        return (zz * ny + yy) * nc + cc

    def step(v, d, n):
        return lax.rem(v + d + n, n)

    def remote(src, dst, send, recv, peer):
        return pltpu.make_async_remote_copy(
            src_ref=src, dst_ref=dst, send_sem=send, recv_sem=recv,
            device_id=peer, device_id_type=MESH,
        )

    def wait_bytes(ref, sem):
        pltpu.make_async_copy(ref, ref, sem).wait()

    right = (e, step(x, 1, nx))
    left = (e, step(x, -1, nx))
    across = (e, step(x, 2, nx))
    y_up = (ep_of(z, step(y, 1, ny), core), x)
    y_dn = (ep_of(z, step(y, -1, ny), core), x)
    z_up = (ep_of(step(z, 1, nz), y, core), x)
    z_dn = (ep_of(step(z, -1, nz), y, core), x)
    twin = (ep_of(z, y, step(core, 1, nc)), x)

    barrier = pltpu.get_barrier_semaphore()
    for peer in (across, right, left):
        pl.semaphore_signal(barrier, inc=1, device_id=peer, device_id_type=MESH)
    z_lo, z_hi, y_lo, y_hi = z == 0, z == nz - 1, y == 0, y == ny - 1
    pairs = (
        (z_up, jnp.logical_not(z_hi)), (z_dn, z_lo),
        (y_up, jnp.logical_not(y_hi)), (y_dn, y_lo),
        (twin, core == 0),
    )
    greeted = sum(g.astype(jnp.int32) for _, g in pairs)

    items = ((0, 0, FIRST), (0, FIRST, width - FIRST), (1, 0, width))
    loads = []
    for i, (t, col, wide) in enumerate(items):
        train, other = ((tg_hbm, og_hbm), (tu_hbm, ou_hbm))[t]
        for h in range(2):
            at = (pl.ds(h * half, half), pl.ds(col, wide))
            pair = (
                pltpu.make_async_copy(train.at[0, *at], lat.at[t, *at], in_sem.at[i, h, 0]),
                pltpu.make_async_copy(other.at[0, *at], oth.at[t, *at], in_sem.at[i, h, 1]),
            )
            for copy in pair:
                copy.start(priority=min(i, 1))
            loads.append(pair)
        if i == 0:
            pltpu.make_async_copy(rw_hbm, rin.at[0], rin_sem).start()
            pltpu.make_async_copy(rg_hbm, rin.at[1], rin_sem).start()

    for peer, greets in pairs:

        @pl.when(greets)
        def _(peer=peer):
            pl.semaphore_signal(barrier, inc=1, device_id=peer, device_id_type=MESH)

    def local_sum(i):
        t, col, wide = items[i]
        cols = pl.ds(col, wide)
        acc = jnp.zeros((8, wide), jnp.float32)
        for h in range(2):
            for copy in loads[2 * i + h]:
                copy.wait()

            def add(j, acc, h=h):
                r = pl.ds(pl.multiple_of(h * half + j * STEP, STEP), STEP)
                v = lat[t, r, cols] + oth[t, r, cols].astype(jnp.float32)
                lat[t, r, cols] = v
                v = v * v
                for k in range(STEP // 8):
                    acc = acc + v[8 * k : 8 * k + 8]
                return acc

            acc = lax.fori_loop(0, half // STEP, add, acc)
        sums[t, x, :, cols] = jnp.sum(acc, axis=0, keepdims=True)

    def spread(piece, send, recv):
        for peer in (across, right, left):
            remote(piece, piece, send, recv, peer).start()

    def send_sum(i):
        t, col, wide = items[i]
        spread(sums.at[t, x, :, pl.ds(col, wide)], sum_send, sum_recv.at[i])

    local_sum(0)
    pl.semaphore_wait(barrier, 3 + len(pairs) - greeted)
    send_sum(0)
    for d, peer in list(enumerate((right, left)))[: 2 * (RAW > 0)]:
        remote(lat.at[0, pl.ds(0, RAW), pl.ds(0, FIRST)], raw.at[d], raw_send, raw_recv, peer).start()
    for peer, greets in pairs:

        @pl.when(jnp.logical_not(greets))
        def _(peer=peer):
            pl.semaphore_signal(answer_sem, inc=1, device_id=peer, device_id_type=MESH)

    for i in range(1, len(items)):
        local_sum(i)
        send_sum(i)
    wait_bytes(rin, rin_sem)
    rx[x] = rin[0] * rin[1]
    spread(rx.at[x], rx_send, rx_recv)

    outs, scales = (out_g, out_u), (scale_g, scale_u)
    inverse = []
    size = half // PIECES
    for i, (t, col, wide) in enumerate(items):
        cols = pl.ds(col, wide)
        wait_bytes(sums.at[t, pl.ds(0, nx - 1), :, cols], sum_recv.at[i])
        total = sums[t, 0, :, cols]
        for k in range(1, nx):
            total = total + sums[t, k, :, cols]
        scale = jnp.sqrt(total)
        scales[t][:, cols] = scale
        inv = jnp.broadcast_to(1.0 / scale, (STEP, wide))
        inverse.append(inv)
        for c in range(2 * PIECES):
            h = c // PIECES
            skip = RAW if i == 0 and c == 0 else 0
            for lo, hi in ((skip, size), (0, skip)):
                if lo == hi:
                    continue

                def narrow(j, carry, t=t, c=c, inv=inv, cols=cols):
                    r = pl.multiple_of(c * size + j * STEP, STEP)
                    w = pl.multiple_of(x * rows + c * size + j * STEP, STEP)
                    outs[t][0, pl.ds(w, STEP), cols] = (lat[t, pl.ds(r, STEP), cols] * inv).astype(jnp.bfloat16)
                    return carry

                lax.fori_loop(lo // STEP, hi // STEP, narrow, 0)
                if lo == skip:
                    where = pl.ds(pl.multiple_of(x * rows + c * size + skip, STEP), size - skip)
                    piece = outs[t].at[0, where, cols]
                    for d, peer in enumerate((right, left)):
                        recv = near_recv.at[d, t] if h == d else rest_recv.at[d]
                        remote(piece, piece, own_send, recv, peer).start()

    if RAW:
        wait_bytes(raw, raw_recv)
    sides = (step(x, -1, nx), step(x, 1, nx))
    for d, source in enumerate(sides):

        def narrow_raw(j, carry, d=d, source=source):
            r = pl.multiple_of(j * STEP, STEP)
            w = pl.multiple_of(source * rows + j * STEP, STEP)
            outs[0][0, pl.ds(w, STEP), pl.ds(0, FIRST)] = (raw[d, pl.ds(r, STEP), :] * inverse[0]).astype(jnp.bfloat16)
            return carry

        lax.fori_loop(0, RAW // STEP, narrow_raw, 0)

    @pl.when(greeted > 0)
    def _():
        pl.semaphore_wait(answer_sem, greeted)

    wait_bytes(rx.at[pl.ds(0, nx - 1)], rx_recv)
    mine = y * nc + core
    plane[mine] = jnp.concatenate([rx[k] for k in range(nx)], axis=1)
    first = remote(plane.at[mine], plane.at[mine], pl_send, pl_recv.at[0], twin)
    first.start()
    first.wait_recv()
    near = pl.ds(y * nc, nc)
    ups = remote(plane.at[near], plane.at[near], pl_send, pl_recv.at[1], y_up)
    dns = remote(plane.at[near], plane.at[near], pl_send, pl_recv.at[2], y_dn)
    ups.start()
    dns.start()
    ups.wait_recv()
    dns.wait_recv()
    from_dn = pl.ds(step(y, -1, ny) * nc, nc)
    far = remote(plane.at[from_dn], plane.at[from_dn], pl_send, pl_recv.at[3], y_up)
    far.start()
    far.wait_recv()
    zring[z] = jnp.concatenate([plane[k] for k in range(ny * nc)], axis=0)
    hops_up, hops_dn = nz // 2, nz - 1 - nz // 2
    for s in range(hops_up):
        at = step(z, -s, nz)
        moves = [remote(zring.at[at], zring.at[at], z_send, z_recv.at[s], z_up)]
        if s < hops_dn:
            at = step(z, s, nz)
            moves.append(remote(zring.at[at], zring.at[at], z_send, z_recv.at[hops_up + s], z_dn))
        for copy in moves:
            copy.start()
        for copy in moves:
            copy.wait_recv()
    for k in range(nz // 2):
        both = jnp.concatenate([zring[2 * k], zring[2 * k + 1]], axis=0)
        router[pl.ds(2 * k * ny * nc, 2 * ny * nc), :] = both.astype(jnp.bfloat16)

    sent_raw = RAW * FIRST // width
    for t in range(2):
        for d, source in enumerate(sides):
            count = half - (sent_raw if t == 0 and d == 0 else 0)
            wait_bytes(outs[t].at[0, pl.ds(0, count)], near_recv.at[d, t])
            where = pl.ds(pl.multiple_of(source * rows + d * half, half), half)
            piece = outs[t].at[0, where]
            remote(piece, piece, fwd_send, fwd_recv, (right, left)[d]).start()
    for d in range(2):
        count = 2 * half - (sent_raw if d == 1 else 0)
        wait_bytes(out_g.at[0, pl.ds(0, count)], rest_recv.at[d])
    wait_bytes(sums.at[:, pl.ds(0, nx - 1)], sum_send)
    wait_bytes(rx.at[pl.ds(0, nx - 1)], rx_send)
    if RAW:
        wait_bytes(raw, raw_send)
    wait_bytes(plane.at[pl.ds(0, 1 + 3 * nc)], pl_send)
    wait_bytes(zring.at[pl.ds(0, nz - 1)], z_send)
    wait_bytes(out_g.at[0, pl.ds(0, 2 * (2 * rows - sent_raw))], own_send)
    wait_bytes(out_g.at[0, pl.ds(0, 4 * half)], fwd_send)
    wait_bytes(out_g.at[0, pl.ds(0, 4 * half)], fwd_recv)


def write_out(*refs):
    held, outs, sem = refs[:5], refs[5:10], refs[10]
    copies = []
    for k in range(2):
        size = held[k].shape[1] // PARTS
        for p in range(PARTS):
            part = (0, pl.ds(p * size, size))
            copies.append(pltpu.make_async_copy(held[k].at[part], outs[k].at[part], sem.at[k * PARTS + p]))
    for k in range(2, 5):
        copies.append(pltpu.make_async_copy(held[k], outs[k], sem.at[2 * PARTS + k - 2]))
    for copy in copies:
        copy.start()
    for copy in copies:
        copy.wait()


def body(dims, train_gate, other_gate, train_up, other_up, router_weight, router_gain):
    nx, ny, nz, nc, rows = dims
    width = train_gate.shape[2]
    whole = nx * rows
    experts = ny * nz * nc
    hbm = pl.BlockSpec(memory_space=pltpu.HBM)
    vmem = pl.BlockSpec(memory_space=pltpu.VMEM)
    dma = pltpu.SemaphoreType.DMA
    out = pl.pallas_call(
        functools.partial(kernel, dims),
        out_shape=(
            pltpu.VMEM((1, whole, width), jnp.bfloat16),
            pltpu.VMEM((1, whole, width), jnp.bfloat16),
            pltpu.VMEM((1, width), jnp.float32),
            pltpu.VMEM((1, width), jnp.float32),
            pltpu.VMEM((experts, whole), jnp.bfloat16),
        ),
        in_specs=[hbm] * 6,
        out_specs=(vmem,) * 5,
        scratch_shapes=[
            pltpu.VMEM((2, rows, width), jnp.float32),
            pltpu.VMEM((2, rows, width), jnp.bfloat16),
            pltpu.VMEM((2, nx, 1, width), jnp.float32),
            pltpu.VMEM((2, max(RAW, STEP), FIRST), jnp.float32),
            pltpu.VMEM((2, 1, rows), jnp.float32),
            pltpu.VMEM((nx, 1, rows), jnp.float32),
            pltpu.VMEM((ny * nc, 1, whole), jnp.float32),
            pltpu.VMEM((nz, ny * nc, whole), jnp.float32),
            dma((3, 2, 2)), dma(()), dma(()), dma((3,)), dma(()), dma(()), dma(()), dma(()),
            dma(()), dma((2, 2)), dma((2,)), dma(()), dma(()),
            dma(()), dma((4,)), dma(()), dma((nz - 1,)),
            pltpu.SemaphoreType.REGULAR,
        ],
        compiler_params=pltpu.CompilerParams(
            collective_id=0, has_side_effects=True, vmem_limit_bytes=48 << 20
        ),
        name="ring",
    )(train_gate, other_gate, train_up, other_up, router_weight.T, router_gain[None, :])
    ready_gate, ready_up, scale_gate, scale_up, router = pl.pallas_call(
        write_out,
        out_shape=tuple(pltpu.HBM(o.shape, o.dtype) for o in out),
        in_specs=[vmem] * 5,
        out_specs=(hbm,) * 5,
        scratch_shapes=[dma((2 * PARTS + 3,))],
        compiler_params=pltpu.CompilerParams(vmem_limit_bytes=4 << 20),
        name="write_out",
    )(*out)
    return ready_gate, ready_up, scale_gate, scale_up, router.T


def solution(mesh):
    placed = (
        P("ep", "fsdp", None),
        P("ep", "fsdp", None),
        P("ep", "fsdp", None),
        P("ep", "fsdp", None),
        P("fsdp", "ep"),
        P("fsdp"),
    )
    nx, ep = mesh.shape["fsdp"], mesh.shape["ep"]
    dims = (nx, 4, ep // 8, 2, 2048 // nx)
    return jax.shard_map(
        functools.partial(body, dims),
        mesh=mesh,
        in_specs=placed,
        out_specs=(P("ep", None, None), P("ep", None, None), P("ep", None), P("ep", None), P()),
        check_vma=False,
    )
```

```python
import functools

import jax
import jax.numpy as jnp
from jax import lax
from jax.experimental import pallas as pl
from jax.experimental.pallas import tpu as pltpu
from jax.sharding import PartitionSpec as P

MESH = pl.DeviceIdType.MESH
STEP = 16
PARTS = 2
RAW = 96
FIRST = 256
PIECES = 1


def kernel(
    dims,
    tg_hbm, og_hbm, tu_hbm, ou_hbm, rw_hbm, rg_hbm,
    out_g, out_u, scale_g, scale_u, router,
    lat, oth, sums, raw, rin, rx, plane, zring,
    in_sem, rin_sem, sum_send, sum_recv, raw_send, raw_recv, rx_send, rx_recv,
    own_send, near_recv, rest_recv, fwd_send, fwd_recv,
    pl_send, pl_recv, z_send, z_recv, answer_sem,
):
    nx, ny, nz, nc, rows = dims
    width = lat.shape[2]
    half = rows // 2
    x = lax.axis_index("fsdp")
    e = lax.axis_index("ep")
    core = lax.rem(e, nc)
    y = lax.rem(lax.div(e, nc), ny)
    z = lax.div(e, nc * ny)

    def ep_of(zz, yy, cc):
        return (zz * ny + yy) * nc + cc

    def step(v, d, n):
        return lax.rem(v + d + n, n)

    def remote(src, dst, send, recv, peer):
        return pltpu.make_async_remote_copy(
            src_ref=src, dst_ref=dst, send_sem=send, recv_sem=recv,
            device_id=peer, device_id_type=MESH,
        )

    def wait_bytes(ref, sem):
        pltpu.make_async_copy(ref, ref, sem).wait()

    right = (e, step(x, 1, nx))
    left = (e, step(x, -1, nx))
    across = (e, step(x, 2, nx))
    y_up = (ep_of(z, step(y, 1, ny), core), x)
    y_dn = (ep_of(z, step(y, -1, ny), core), x)
    z_up = (ep_of(step(z, 1, nz), y, core), x)
    z_dn = (ep_of(step(z, -1, nz), y, core), x)
    twin = (ep_of(z, y, step(core, 1, nc)), x)

    barrier = pltpu.get_barrier_semaphore()
    for peer in (across, right, left):
        pl.semaphore_signal(barrier, inc=1, device_id=peer, device_id_type=MESH)
    z_lo, z_hi, y_lo, y_hi = z == 0, z == nz - 1, y == 0, y == ny - 1
    pairs = (
        (z_up, jnp.logical_not(z_hi)), (z_dn, z_lo),
        (y_up, jnp.logical_not(y_hi)), (y_dn, y_lo),
        (twin, core == 0),
    )
    greeted = sum(g.astype(jnp.int32) for _, g in pairs)

    items = ((0, 0, FIRST), (0, FIRST, width - FIRST), (1, 0, width))
    loads = []
    for i, (t, col, wide) in enumerate(items):
        train, other = ((tg_hbm, og_hbm), (tu_hbm, ou_hbm))[t]
        for h in range(2):
            at = (pl.ds(h * half, half), pl.ds(col, wide))
            pair = (
                pltpu.make_async_copy(train.at[0, *at], lat.at[t, *at], in_sem.at[i, h, 0]),
                pltpu.make_async_copy(other.at[0, *at], oth.at[t, *at], in_sem.at[i, h, 1]),
            )
            for copy in pair:
                copy.start()
            loads.append(pair)
        if i == 0:
            pltpu.make_async_copy(rw_hbm, rin.at[0], rin_sem).start()
            pltpu.make_async_copy(rg_hbm, rin.at[1], rin_sem).start()

    for peer, greets in pairs:

        @pl.when(greets)
        def _(peer=peer):
            pl.semaphore_signal(barrier, inc=1, device_id=peer, device_id_type=MESH)

    def local_sum(i):
        t, col, wide = items[i]
        cols = pl.ds(col, wide)
        acc = jnp.zeros((8, wide), jnp.float32)
        for h in range(2):
            for copy in loads[2 * i + h]:
                copy.wait()

            def add(j, acc, h=h):
                r = pl.ds(pl.multiple_of(h * half + j * STEP, STEP), STEP)
                v = lat[t, r, cols] + oth[t, r, cols].astype(jnp.float32)
                lat[t, r, cols] = v
                v = v * v
                for k in range(STEP // 8):
                    acc = acc + v[8 * k : 8 * k + 8]
                return acc

            acc = lax.fori_loop(0, half // STEP, add, acc)
        sums[t, x, :, cols] = jnp.sum(acc, axis=0, keepdims=True)

    def spread(piece, send, recv):
        for peer in (across, right, left):
            remote(piece, piece, send, recv, peer).start()

    def send_sum(i):
        t, col, wide = items[i]
        spread(sums.at[t, x, :, pl.ds(col, wide)], sum_send, sum_recv.at[i])

    local_sum(0)
    pl.semaphore_wait(barrier, 3 + len(pairs) - greeted)
    send_sum(0)
    for d, peer in enumerate((right, left)):
        remote(lat.at[0, pl.ds(0, RAW), pl.ds(0, FIRST)], raw.at[d], raw_send, raw_recv, peer).start()
    for peer, greets in pairs:

        @pl.when(jnp.logical_not(greets))
        def _(peer=peer):
            pl.semaphore_signal(answer_sem, inc=1, device_id=peer, device_id_type=MESH)

    for i in range(1, len(items)):
        local_sum(i)
        send_sum(i)
    wait_bytes(rin, rin_sem)
    rx[x] = rin[0] * rin[1]
    spread(rx.at[x], rx_send, rx_recv)

    outs, scales = (out_g, out_u), (scale_g, scale_u)
    inverse = []
    size = half // PIECES
    for i, (t, col, wide) in enumerate(items):
        cols = pl.ds(col, wide)
        wait_bytes(sums.at[t, pl.ds(0, nx - 1), :, cols], sum_recv.at[i])
        total = sums[t, 0, :, cols]
        for k in range(1, nx):
            total = total + sums[t, k, :, cols]
        scale = jnp.sqrt(total)
        scales[t][:, cols] = scale
        inv = jnp.broadcast_to(1.0 / scale, (STEP, wide))
        inverse.append(inv)
        for c in range(2 * PIECES):
            h = c // PIECES
            skip = RAW if i == 0 and c == 0 else 0
            for lo, hi in ((skip, size), (0, skip)):
                if lo == hi:
                    continue

                def narrow(j, carry, t=t, c=c, inv=inv, cols=cols):
                    r = pl.multiple_of(c * size + j * STEP, STEP)
                    w = pl.multiple_of(x * rows + c * size + j * STEP, STEP)
                    outs[t][0, pl.ds(w, STEP), cols] = (lat[t, pl.ds(r, STEP), cols] * inv).astype(jnp.bfloat16)
                    return carry

                lax.fori_loop(lo // STEP, hi // STEP, narrow, 0)
                if lo == skip:
                    where = pl.ds(pl.multiple_of(x * rows + c * size + skip, STEP), size - skip)
                    piece = outs[t].at[0, where, cols]
                    for d, peer in enumerate((right, left)):
                        recv = near_recv.at[d, t] if h == d else rest_recv.at[d]
                        remote(piece, piece, own_send, recv, peer).start()

    wait_bytes(raw, raw_recv)
    sides = (step(x, -1, nx), step(x, 1, nx))
    for d, source in enumerate(sides):

        def narrow_raw(j, carry, d=d, source=source):
            r = pl.multiple_of(j * STEP, STEP)
            w = pl.multiple_of(source * rows + j * STEP, STEP)
            outs[0][0, pl.ds(w, STEP), pl.ds(0, FIRST)] = (raw[d, pl.ds(r, STEP), :] * inverse[0]).astype(jnp.bfloat16)
            return carry

        lax.fori_loop(0, RAW // STEP, narrow_raw, 0)

    @pl.when(greeted > 0)
    def _():
        pl.semaphore_wait(answer_sem, greeted)

    wait_bytes(rx.at[pl.ds(0, nx - 1)], rx_recv)
    mine = y * nc + core
    plane[mine] = jnp.concatenate([rx[k] for k in range(nx)], axis=1)
    first = remote(plane.at[mine], plane.at[mine], pl_send, pl_recv.at[0], twin)
    first.start()
    first.wait_recv()
    near = pl.ds(y * nc, nc)
    ups = remote(plane.at[near], plane.at[near], pl_send, pl_recv.at[1], y_up)
    dns = remote(plane.at[near], plane.at[near], pl_send, pl_recv.at[2], y_dn)
    ups.start()
    dns.start()
    ups.wait_recv()
    dns.wait_recv()
    from_dn = pl.ds(step(y, -1, ny) * nc, nc)
    far = remote(plane.at[from_dn], plane.at[from_dn], pl_send, pl_recv.at[3], y_up)
    far.start()
    far.wait_recv()
    zring[z] = jnp.concatenate([plane[k] for k in range(ny * nc)], axis=0)
    hops_up, hops_dn = nz // 2, nz - 1 - nz // 2
    for s in range(hops_up):
        at = step(z, -s, nz)
        moves = [remote(zring.at[at], zring.at[at], z_send, z_recv.at[s], z_up)]
        if s < hops_dn:
            at = step(z, s, nz)
            moves.append(remote(zring.at[at], zring.at[at], z_send, z_recv.at[hops_up + s], z_dn))
        for copy in moves:
            copy.start()
        for copy in moves:
            copy.wait_recv()
    for k in range(nz // 2):
        both = jnp.concatenate([zring[2 * k], zring[2 * k + 1]], axis=0)
        router[pl.ds(2 * k * ny * nc, 2 * ny * nc), :] = both.astype(jnp.bfloat16)

    sent_raw = RAW * FIRST // width
    for t in range(2):
        for d, source in enumerate(sides):
            count = half - (sent_raw if t == 0 and d == 0 else 0)
            wait_bytes(outs[t].at[0, pl.ds(0, count)], near_recv.at[d, t])
            where = pl.ds(pl.multiple_of(source * rows + d * half, half), half)
            piece = outs[t].at[0, where]
            remote(piece, piece, fwd_send, fwd_recv, (right, left)[d]).start()
    for d in range(2):
        count = 2 * half - (sent_raw if d == 1 else 0)
        wait_bytes(out_g.at[0, pl.ds(0, count)], rest_recv.at[d])
    wait_bytes(sums.at[:, pl.ds(0, nx - 1)], sum_send)
    wait_bytes(rx.at[pl.ds(0, nx - 1)], rx_send)
    wait_bytes(raw, raw_send)
    wait_bytes(plane.at[pl.ds(0, 1 + 3 * nc)], pl_send)
    wait_bytes(zring.at[pl.ds(0, nz - 1)], z_send)
    wait_bytes(out_g.at[0, pl.ds(0, 2 * (2 * rows - sent_raw))], own_send)
    wait_bytes(out_g.at[0, pl.ds(0, 4 * half)], fwd_send)
    wait_bytes(out_g.at[0, pl.ds(0, 4 * half)], fwd_recv)


def write_out(*refs):
    held, outs, sem = refs[:5], refs[5:10], refs[10]
    copies = []
    for k in range(2):
        size = held[k].shape[1] // PARTS
        for p in range(PARTS):
            part = (0, pl.ds(p * size, size))
            copies.append(pltpu.make_async_copy(held[k].at[part], outs[k].at[part], sem.at[k * PARTS + p]))
    for k in range(2, 5):
        copies.append(pltpu.make_async_copy(held[k], outs[k], sem.at[2 * PARTS + k - 2]))
    for copy in copies:
        copy.start()
    for copy in copies:
        copy.wait()


def body(dims, train_gate, other_gate, train_up, other_up, router_weight, router_gain):
    nx, ny, nz, nc, rows = dims
    width = train_gate.shape[2]
    whole = nx * rows
    experts = ny * nz * nc
    hbm = pl.BlockSpec(memory_space=pltpu.HBM)
    vmem = pl.BlockSpec(memory_space=pltpu.VMEM)
    dma = pltpu.SemaphoreType.DMA
    out = pl.pallas_call(
        functools.partial(kernel, dims),
        out_shape=(
            pltpu.VMEM((1, whole, width), jnp.bfloat16),
            pltpu.VMEM((1, whole, width), jnp.bfloat16),
            pltpu.VMEM((1, width), jnp.float32),
            pltpu.VMEM((1, width), jnp.float32),
            pltpu.VMEM((experts, whole), jnp.bfloat16),
        ),
        in_specs=[hbm] * 6,
        out_specs=(vmem,) * 5,
        scratch_shapes=[
            pltpu.VMEM((2, rows, width), jnp.float32),
            pltpu.VMEM((2, rows, width), jnp.bfloat16),
            pltpu.VMEM((2, nx, 1, width), jnp.float32),
            pltpu.VMEM((2, RAW, FIRST), jnp.float32),
            pltpu.VMEM((2, 1, rows), jnp.float32),
            pltpu.VMEM((nx, 1, rows), jnp.float32),
            pltpu.VMEM((ny * nc, 1, whole), jnp.float32),
            pltpu.VMEM((nz, ny * nc, whole), jnp.float32),
            dma((3, 2, 2)), dma(()), dma(()), dma((3,)), dma(()), dma(()), dma(()), dma(()),
            dma(()), dma((2, 2)), dma((2,)), dma(()), dma(()),
            dma(()), dma((4,)), dma(()), dma((nz - 1,)),
            pltpu.SemaphoreType.REGULAR,
        ],
        compiler_params=pltpu.CompilerParams(
            collective_id=0, has_side_effects=True, vmem_limit_bytes=48 << 20
        ),
        name="ring",
    )(train_gate, other_gate, train_up, other_up, router_weight.T, router_gain[None, :])
    ready_gate, ready_up, scale_gate, scale_up, router = pl.pallas_call(
        write_out,
        out_shape=tuple(pltpu.HBM(o.shape, o.dtype) for o in out),
        in_specs=[vmem] * 5,
        out_specs=(hbm,) * 5,
        scratch_shapes=[dma((2 * PARTS + 3,))],
        compiler_params=pltpu.CompilerParams(vmem_limit_bytes=4 << 20),
        name="write_out",
    )(*out)
    return ready_gate, ready_up, scale_gate, scale_up, router.T


def solution(mesh):
    placed = (
        P("ep", "fsdp", None),
        P("ep", "fsdp", None),
        P("ep", "fsdp", None),
        P("ep", "fsdp", None),
        P("fsdp", "ep"),
        P("fsdp"),
    )
    nx, ep = mesh.shape["fsdp"], mesh.shape["ep"]
    dims = (nx, 4, ep // 8, 2, 2048 // nx)
    return jax.shard_map(
        functools.partial(body, dims),
        mesh=mesh,
        in_specs=placed,
        out_specs=(P("ep", None, None), P("ep", None, None), P("ep", None), P("ep", None), P()),
        check_vma=False,
    )
```

```python
import functools

import jax
import jax.numpy as jnp
from jax import lax
from jax.experimental import pallas as pl
from jax.experimental.pallas import tpu as pltpu
from jax.sharding import PartitionSpec as P

MESH = pl.DeviceIdType.MESH
STEP = 16
PARTS = 2
RAW = 96
FIRST = 256
PIECES = 1


def kernel(
    dims,
    tg_hbm, og_hbm, tu_hbm, ou_hbm, rw_hbm, rg_hbm,
    out_g, out_u, scale_g, scale_u, router,
    lat, oth, sums, raw, rin, rx, plane, zring,
    in_sem, rin_sem, sum_send, sum_recv, raw_send, raw_recv, rx_send, rx_recv,
    own_send, near_recv, rest_recv, fwd_send, fwd_recv,
    pl_send, pl_recv, z_send, z_recv, answer_sem,
):
    nx, ny, nz, nc, rows = dims
    width = lat.shape[2]
    half = rows // 2
    x = lax.axis_index("fsdp")
    e = lax.axis_index("ep")
    core = lax.rem(e, nc)
    y = lax.rem(lax.div(e, nc), ny)
    z = lax.div(e, nc * ny)

    def ep_of(zz, yy, cc):
        return (zz * ny + yy) * nc + cc

    def step(v, d, n):
        return lax.rem(v + d + n, n)

    def remote(src, dst, send, recv, peer):
        return pltpu.make_async_remote_copy(
            src_ref=src, dst_ref=dst, send_sem=send, recv_sem=recv,
            device_id=peer, device_id_type=MESH,
        )

    def wait_bytes(ref, sem):
        pltpu.make_async_copy(ref, ref, sem).wait()

    right = (e, step(x, 1, nx))
    left = (e, step(x, -1, nx))
    across = (e, step(x, 2, nx))
    y_up = (ep_of(z, step(y, 1, ny), core), x)
    y_dn = (ep_of(z, step(y, -1, ny), core), x)
    z_up = (ep_of(step(z, 1, nz), y, core), x)
    z_dn = (ep_of(step(z, -1, nz), y, core), x)
    twin = (ep_of(z, y, step(core, 1, nc)), x)

    barrier = pltpu.get_barrier_semaphore()
    for peer in (across, right, left):
        pl.semaphore_signal(barrier, inc=1, device_id=peer, device_id_type=MESH)
    z_lo, z_hi, y_lo, y_hi = z == 0, z == nz - 1, y == 0, y == ny - 1
    pairs = (
        (z_up, jnp.logical_not(z_hi)), (z_dn, z_lo),
        (y_up, jnp.logical_not(y_hi)), (y_dn, y_lo),
        (twin, core == 0),
    )
    greeted = sum(g.astype(jnp.int32) for _, g in pairs)

    items = ((0, 0, FIRST), (0, FIRST, width - FIRST), (1, 0, width))
    loads = []
    for i, (t, col, wide) in enumerate(items):
        train, other = ((tg_hbm, og_hbm), (tu_hbm, ou_hbm))[t]
        parts = 2 if i == 0 else 1
        deep = rows // parts
        for h in range(parts):
            at = (pl.ds(h * deep, deep), pl.ds(col, wide))
            pair = (
                pltpu.make_async_copy(train.at[0, *at], lat.at[t, *at], in_sem.at[i + h if i == 0 else i + 1, 0]),
                pltpu.make_async_copy(other.at[0, *at], oth.at[t, *at], in_sem.at[i + h if i == 0 else i + 1, 1]),
            )
            for copy in pair:
                copy.start()
            loads.append((i, h, deep, pair))
        if i == 0:
            pltpu.make_async_copy(rw_hbm, rin.at[0], rin_sem).start()
            pltpu.make_async_copy(rg_hbm, rin.at[1], rin_sem).start()

    for peer, greets in pairs:

        @pl.when(greets)
        def _(peer=peer):
            pl.semaphore_signal(barrier, inc=1, device_id=peer, device_id_type=MESH)

    def local_sum(i):
        t, col, wide = items[i]
        cols = pl.ds(col, wide)
        acc = jnp.zeros((8, wide), jnp.float32)
        for _, h, deep, pair in [load for load in loads if load[0] == i]:
            for copy in pair:
                copy.wait()

            def add(j, acc, first=h * deep):
                r = pl.ds(pl.multiple_of(first + j * STEP, STEP), STEP)
                v = lat[t, r, cols] + oth[t, r, cols].astype(jnp.float32)
                lat[t, r, cols] = v
                v = v * v
                for k in range(STEP // 8):
                    acc = acc + v[8 * k : 8 * k + 8]
                return acc

            acc = lax.fori_loop(0, deep // STEP, add, acc)
        sums[t, x, :, cols] = jnp.sum(acc, axis=0, keepdims=True)

    def spread(piece, send, recv):
        for peer in (across, right, left):
            remote(piece, piece, send, recv, peer).start()

    def send_sum(i):
        t, col, wide = items[i]
        spread(sums.at[t, x, :, pl.ds(col, wide)], sum_send, sum_recv.at[i])

    local_sum(0)
    pl.semaphore_wait(barrier, 3 + len(pairs) - greeted)
    send_sum(0)
    for d, peer in enumerate((right, left)):
        remote(lat.at[0, pl.ds(0, RAW), pl.ds(0, FIRST)], raw.at[d], raw_send, raw_recv, peer).start()
    for peer, greets in pairs:

        @pl.when(jnp.logical_not(greets))
        def _(peer=peer):
            pl.semaphore_signal(answer_sem, inc=1, device_id=peer, device_id_type=MESH)

    for i in range(1, len(items)):
        local_sum(i)
        send_sum(i)
    wait_bytes(rin, rin_sem)
    rx[x] = rin[0] * rin[1]
    spread(rx.at[x], rx_send, rx_recv)

    outs, scales = (out_g, out_u), (scale_g, scale_u)
    inverse = []
    size = half // PIECES
    for i, (t, col, wide) in enumerate(items):
        cols = pl.ds(col, wide)
        wait_bytes(sums.at[t, pl.ds(0, nx - 1), :, cols], sum_recv.at[i])
        total = sums[t, 0, :, cols]
        for k in range(1, nx):
            total = total + sums[t, k, :, cols]
        scale = jnp.sqrt(total)
        scales[t][:, cols] = scale
        inv = jnp.broadcast_to(1.0 / scale, (STEP, wide))
        inverse.append(inv)
        for c in range(2 * PIECES):
            h = c // PIECES
            skip = RAW if i == 0 and c == 0 else 0
            for lo, hi in ((skip, size), (0, skip)):
                if lo == hi:
                    continue

                def narrow(j, carry, t=t, c=c, inv=inv, cols=cols):
                    r = pl.multiple_of(c * size + j * STEP, STEP)
                    w = pl.multiple_of(x * rows + c * size + j * STEP, STEP)
                    outs[t][0, pl.ds(w, STEP), cols] = (lat[t, pl.ds(r, STEP), cols] * inv).astype(jnp.bfloat16)
                    return carry

                lax.fori_loop(lo // STEP, hi // STEP, narrow, 0)
                if lo == skip:
                    where = pl.ds(pl.multiple_of(x * rows + c * size + skip, STEP), size - skip)
                    piece = outs[t].at[0, where, cols]
                    for d, peer in enumerate((right, left)):
                        recv = near_recv.at[d, t] if h == d else rest_recv
                        remote(piece, piece, own_send, recv, peer).start()

    wait_bytes(raw, raw_recv)
    sides = (step(x, -1, nx), step(x, 1, nx))
    for d, source in enumerate(sides):

        def narrow_raw(j, carry, d=d, source=source):
            r = pl.multiple_of(j * STEP, STEP)
            w = pl.multiple_of(source * rows + j * STEP, STEP)
            outs[0][0, pl.ds(w, STEP), pl.ds(0, FIRST)] = (raw[d, pl.ds(r, STEP), :] * inverse[0]).astype(jnp.bfloat16)
            return carry

        lax.fori_loop(0, RAW // STEP, narrow_raw, 0)

    @pl.when(greeted > 0)
    def _():
        pl.semaphore_wait(answer_sem, greeted)

    wait_bytes(rx.at[pl.ds(0, nx - 1)], rx_recv)
    mine = y * nc + core
    plane[mine] = jnp.concatenate([rx[k] for k in range(nx)], axis=1)
    first = remote(plane.at[mine], plane.at[mine], pl_send, pl_recv.at[0], twin)
    first.start()
    first.wait_recv()
    near = pl.ds(y * nc, nc)
    ups = remote(plane.at[near], plane.at[near], pl_send, pl_recv.at[1], y_up)
    dns = remote(plane.at[near], plane.at[near], pl_send, pl_recv.at[1], y_dn)
    ups.start()
    dns.start()
    wait_bytes(plane.at[pl.ds(0, 2 * nc)], pl_recv.at[1])
    from_dn = pl.ds(step(y, -1, ny) * nc, nc)
    far = remote(plane.at[from_dn], plane.at[from_dn], pl_send, pl_recv.at[2], y_up)
    far.start()
    far.wait_recv()
    zring[z] = jnp.concatenate([plane[k] for k in range(ny * nc)], axis=0)
    hops_up, hops_dn = nz // 2, nz - 1 - nz // 2
    for s in range(hops_up):
        at = step(z, -s, nz)
        moves = [remote(zring.at[at], zring.at[at], z_send, z_recv.at[s], z_up)]
        if s < hops_dn:
            at = step(z, s, nz)
            moves.append(remote(zring.at[at], zring.at[at], z_send, z_recv.at[s], z_dn))
        for copy in moves:
            copy.start()
        wait_bytes(zring.at[pl.ds(0, len(moves))], z_recv.at[s])
    for k in range(nz // 2):
        both = jnp.concatenate([zring[2 * k], zring[2 * k + 1]], axis=0)
        router[pl.ds(2 * k * ny * nc, 2 * ny * nc), :] = both.astype(jnp.bfloat16)

    sent_raw = RAW * FIRST // width
    for t in range(2):
        for d, source in enumerate(sides):
            count = half - (sent_raw if t == 0 and d == 0 else 0)
            wait_bytes(outs[t].at[0, pl.ds(0, count)], near_recv.at[d, t])
            where = pl.ds(pl.multiple_of(source * rows + d * half, half), half)
            piece = outs[t].at[0, where]
            remote(piece, piece, fwd_send, fwd_recv, (right, left)[d]).start()
    wait_bytes(out_g.at[0, pl.ds(0, 4 * half - sent_raw)], rest_recv)
    wait_bytes(sums.at[:, pl.ds(0, nx - 1)], sum_send)
    wait_bytes(rx.at[pl.ds(0, nx - 1)], rx_send)
    wait_bytes(raw, raw_send)
    wait_bytes(plane.at[pl.ds(0, 1 + 3 * nc)], pl_send)
    wait_bytes(zring.at[pl.ds(0, nz - 1)], z_send)
    wait_bytes(out_g.at[0, pl.ds(0, 2 * (2 * rows - sent_raw))], own_send)
    wait_bytes(out_g.at[0, pl.ds(0, 4 * half)], fwd_send)
    wait_bytes(out_g.at[0, pl.ds(0, 4 * half)], fwd_recv)


def write_out(*refs):
    held, outs, sem = refs[:5], refs[5:10], refs[10]
    copies = []
    for k in range(2):
        size = held[k].shape[1] // PARTS
        for p in range(PARTS):
            part = (0, pl.ds(p * size, size))
            copies.append(pltpu.make_async_copy(held[k].at[part], outs[k].at[part], sem.at[k * PARTS + p]))
    for k in range(2, 5):
        copies.append(pltpu.make_async_copy(held[k], outs[k], sem.at[2 * PARTS + k - 2]))
    for copy in copies:
        copy.start()
    for copy in copies:
        copy.wait()


def body(dims, train_gate, other_gate, train_up, other_up, router_weight, router_gain):
    nx, ny, nz, nc, rows = dims
    width = train_gate.shape[2]
    whole = nx * rows
    experts = ny * nz * nc
    hbm = pl.BlockSpec(memory_space=pltpu.HBM)
    vmem = pl.BlockSpec(memory_space=pltpu.VMEM)
    dma = pltpu.SemaphoreType.DMA
    out = pl.pallas_call(
        functools.partial(kernel, dims),
        out_shape=(
            pltpu.VMEM((1, whole, width), jnp.bfloat16),
            pltpu.VMEM((1, whole, width), jnp.bfloat16),
            pltpu.VMEM((1, width), jnp.float32),
            pltpu.VMEM((1, width), jnp.float32),
            pltpu.VMEM((experts, whole), jnp.bfloat16),
        ),
        in_specs=[hbm] * 6,
        out_specs=(vmem,) * 5,
        scratch_shapes=[
            pltpu.VMEM((2, rows, width), jnp.float32),
            pltpu.VMEM((2, rows, width), jnp.bfloat16),
            pltpu.VMEM((2, nx, 1, width), jnp.float32),
            pltpu.VMEM((2, RAW, FIRST), jnp.float32),
            pltpu.VMEM((2, 1, rows), jnp.float32),
            pltpu.VMEM((nx, 1, rows), jnp.float32),
            pltpu.VMEM((ny * nc, 1, whole), jnp.float32),
            pltpu.VMEM((nz, ny * nc, whole), jnp.float32),
            dma((4, 2)), dma(()), dma(()), dma((3,)), dma(()), dma(()), dma(()), dma(()),
            dma(()), dma((2, 2)), dma(()), dma(()), dma(()),
            dma(()), dma((3,)), dma(()), dma((nz // 2,)),
            pltpu.SemaphoreType.REGULAR,
        ],
        compiler_params=pltpu.CompilerParams(
            collective_id=0, has_side_effects=True, vmem_limit_bytes=48 << 20
        ),
        name="ring",
    )(train_gate, other_gate, train_up, other_up, router_weight.T, router_gain[None, :])
    ready_gate, ready_up, scale_gate, scale_up, router = pl.pallas_call(
        write_out,
        out_shape=tuple(pltpu.HBM(o.shape, o.dtype) for o in out),
        in_specs=[vmem] * 5,
        out_specs=(hbm,) * 5,
        scratch_shapes=[dma((2 * PARTS + 3,))],
        compiler_params=pltpu.CompilerParams(vmem_limit_bytes=4 << 20),
        name="write_out",
    )(*out)
    return ready_gate, ready_up, scale_gate, scale_up, router.T


def solution(mesh):
    placed = (
        P("ep", "fsdp", None),
        P("ep", "fsdp", None),
        P("ep", "fsdp", None),
        P("ep", "fsdp", None),
        P("fsdp", "ep"),
        P("fsdp"),
    )
    nx, ep = mesh.shape["fsdp"], mesh.shape["ep"]
    dims = (nx, 4, ep // 8, 2, 2048 // nx)
    return jax.shard_map(
        functools.partial(body, dims),
        mesh=mesh,
        in_specs=placed,
        out_specs=(P("ep", None, None), P("ep", None, None), P("ep", None), P("ep", None), P()),
        check_vma=False,
    )
```
